64 devices in a mesh: dp: 4 (over x, y), sp: 16 (over z, core).
Axes of the slice: x: 2, y: 2, z: 8, core: 2. Of those that a mesh axis runs over, the one named last changes fastest.
The devices are a block of a 4x4x8 slice.
Arguments:
- patches: bfloat16 [64, 8192, 512], P('dp', 'sp'), parts along dimension 0
- ln1_scale: float32 [512], replicated
- ln1_bias: float32 [512], replicated
- w_tok1: bfloat16 [8192, 256], replicated
- b_tok1: float32 [256], replicated
- w_tok2: bfloat16 [256, 8192], replicated
- b_tok2: float32 [8192], replicated
- ln2_scale: float32 [512], replicated
- ln2_bias: float32 [512], replicated
- w_ch1: bfloat16 [512, 2048], replicated
- b_ch1: float32 [2048], replicated
- w_ch2: bfloat16 [2048, 512], replicated
- b_ch2: float32 [512], replicated
Outputs:
- output: bfloat16 [64, 8192, 512], P('dp', 'sp'), parts along dimension 0
There are 4 independent parts. The reference program is written for one: setup_inputs(seed, part) draws one part's arguments, and reference() takes and returns one part's arrays. A program takes and returns all parts, laid end to end along the dimension named above; an argument that names none is the same for every part.
All inputs are finite; a program needn't handle non-finite values.
Results may differ from the reference program's by a relative error of at most 0.0111177.
Values are sent between devices in bfloat16 or wider.
A program may use at most 768 MiB of HBM per device.

```python
import jax
import jax.numpy as jnp
from jax import lax

BATCH = 16
SEQ_DEV = 512
GROUP = 16
CHANNELS = 512
TOK_HIDDEN = 256
CH_HIDDEN = 2048
SEQ_LEN = SEQ_DEV * GROUP
LN_EPS = 1e-6


def layer_norm(rows, scale, offset):
    rows_wide = rows.astype(jnp.float32)
    row_mean = jnp.mean(rows_wide, axis=-1, keepdims=True)
    centered = rows_wide - row_mean
    row_var = jnp.mean(centered * centered, axis=-1, keepdims=True)
    return (centered * lax.rsqrt(row_var + LN_EPS) * scale + offset).astype(jnp.bfloat16)


def setup_inputs(seed: int = 0, part: int = 0) -> dict:
    keys = jax.random.split(jax.random.key(seed), 13)

    def draw_normal(index, shape):
        return jax.random.normal(keys[index], shape, jnp.float32)

    patches = jax.random.normal(jax.random.fold_in(keys[0], part), (BATCH, SEQ_LEN, CHANNELS), jnp.float32)
    return dict(
        patches=patches.astype(jnp.bfloat16),
        ln1_scale=1.0 + 0.3 * draw_normal(1, (CHANNELS,)),
        ln1_bias=0.3 * draw_normal(2, (CHANNELS,)),
        w_tok1=(draw_normal(3, (SEQ_LEN, TOK_HIDDEN)) * SEQ_LEN ** -0.5).astype(jnp.bfloat16),
        b_tok1=0.5 * draw_normal(4, (TOK_HIDDEN,)),
        w_tok2=(draw_normal(5, (TOK_HIDDEN, SEQ_LEN)) * TOK_HIDDEN ** -0.5).astype(jnp.bfloat16),
        b_tok2=0.5 * draw_normal(6, (SEQ_LEN,)),
        ln2_scale=1.0 + 0.3 * draw_normal(7, (CHANNELS,)),
        ln2_bias=0.3 * draw_normal(8, (CHANNELS,)),
        w_ch1=(draw_normal(9, (CHANNELS, CH_HIDDEN)) * CHANNELS ** -0.5).astype(jnp.bfloat16),
        b_ch1=0.5 * draw_normal(10, (CH_HIDDEN,)),
        w_ch2=(draw_normal(11, (CH_HIDDEN, CHANNELS)) * CH_HIDDEN ** -0.5).astype(jnp.bfloat16),
        b_ch2=0.5 * draw_normal(12, (CHANNELS,)),
    )


def reference(patches, ln1_scale, ln1_bias, w_tok1, b_tok1, w_tok2, b_tok2, ln2_scale, ln2_bias, w_ch1, b_ch1, w_ch2, b_ch2):
    w_tok2_blocks = jnp.transpose(w_tok2.reshape(TOK_HIDDEN, GROUP, SEQ_DEV), (1, 0, 2))
    b_tok2_blocks = b_tok2.reshape(GROUP, SEQ_DEV)

    def one_image(image):
        normed = layer_norm(image, ln1_scale, ln1_bias)
        hidden = jnp.dot(w_tok1.T, normed, preferred_element_type=jnp.float32) + b_tok1[:, None]
        act_tok = jax.nn.gelu(hidden, approximate=True).astype(jnp.bfloat16)
        image_blocks = image.reshape(GROUP, SEQ_DEV, CHANNELS)

        def one_block(block_args):
            rows, w_rows, b_rows = block_args
            mixed = (jnp.dot(w_rows.T, act_tok, preferred_element_type=jnp.float32) + b_rows[:, None]).astype(jnp.bfloat16)
            residual = (rows.astype(jnp.float32) + mixed.astype(jnp.float32)).astype(jnp.bfloat16)
            chan_in = layer_norm(residual, ln2_scale, ln2_bias)
            pre_act = jnp.dot(chan_in, w_ch1, preferred_element_type=jnp.float32) + b_ch1
            act_ch = jax.nn.gelu(pre_act, approximate=True).astype(jnp.bfloat16)
            ch_out = jnp.dot(act_ch, w_ch2, preferred_element_type=jnp.float32) + b_ch2
            return (residual.astype(jnp.float32) + ch_out).astype(jnp.bfloat16)

        out_blocks = lax.map(one_block, (image_blocks, w_tok2_blocks, b_tok2_blocks))
        return out_blocks.reshape(SEQ_LEN, CHANNELS)

    return lax.map(one_image, patches)
```

```python
import functools

import jax
import jax.numpy as jnp
from jax import lax
from jax.experimental import pallas as pl
from jax.experimental.pallas import tpu as pltpu
from jax.sharding import PartitionSpec as P

LN_EPS = 1e-6
GELU_K = 0.7978845608028654
F32 = jnp.float32
BF16 = jnp.bfloat16
VMEM_LIMIT = 67043328


def layer_norm(wide, scale, offset):
    mean = jnp.mean(wide, axis=-1, keepdims=True)
    centered = wide - mean
    var = jnp.mean(centered * centered, axis=-1, keepdims=True)
    return (centered * lax.rsqrt(var + LN_EPS) * scale + offset).astype(BF16)


def gelu_of_half(half):
    inner = half * (half * half * (8.0 * 0.044715 * GELU_K) + 2.0 * GELU_K)
    return half + half * jnp.tanh(inner)


def lanes(col, width):
    return jnp.concatenate([col] * (width // 128), axis=1)


def column(row):
    return jnp.broadcast_to(row, (128, row.shape[1])).T


def norm_and_project(x_img, ln1s, ln1b, wt1t, u_s, h_img):
    seq, ch = u_s.shape
    step = 128
    for r in range(0, seq, step):
        u_s[r:r + step, :] = layer_norm(x_img[r:r + step, :].astype(F32), ln1s[...], ln1b[...])
    h_img[...] = jnp.dot(wt1t[...], u_s[...], preferred_element_type=F32)


def token_out_and_channel_mix(x_img, g_img, wt2t, bcol2, ln2s, ln2b, w1, b1h, w2, b2, x1_s, v_s, q_s, o_img, rows=256, wide=512):
    seq, ch = v_s.shape
    hid = w1.shape[1]
    for r in range(0, seq, rows):
        rs = slice(r, r + rows)
        mixed = jnp.dot(wt2t[rs, :], g_img[...], preferred_element_type=F32)
        mixed = (mixed + lanes(bcol2[rs, :], ch)).astype(BF16)
        x1 = (x_img[rs, :].astype(F32) + mixed.astype(F32)).astype(BF16)
        x1_s[rs, :] = x1
        v_s[rs, :] = layer_norm(x1.astype(F32), ln2s[...], ln2b[...])
        for e in range(0, hid, wide):
            es = slice(e, e + wide)
            half = jnp.dot(v_s[rs, :], w1[:, es], preferred_element_type=F32) + b1h[:, es]
            q_s[rs, es] = gelu_of_half(half).astype(BF16)
        y = jnp.dot(q_s[rs, :], w2[...], preferred_element_type=F32) + b2[...]
        o_img[rs, :] = (x1_s[rs, :].astype(F32) + y).astype(BF16)


def fused_kernel(nz, x_hbm, ln1s, ln1b, wt1_hbm, bt1, wt2_hbm, bt2, ln2s, ln2b, w1_hbm, b1, w2_hbm, b2, out_hbm,
                 x_v, h_v, d2d_v, rs_v, g_v, wt1_v, wt1t, wt2_v, wt2t, bcol1, bcol2, w1, w2, b1h, u_s, x1_s, v_s, q_s, o_v,
                 x_sem, w_sem, o_sem, send_sem, dr_sem, rr_sem, ar_sem, gr_sem):
    units, seq, ch = x_v.shape
    tok_hid = h_v.shape[1]
    hid = w1.shape[1]
    half_rows = tok_hid // 2
    piece = half_rows // nz
    hop = nz // 2
    me = lax.axis_index('sp')
    z = lax.div(me, 2)
    c = lax.rem(me, 2)
    right = lax.rem(z + 1, nz) * 2 + c
    left = lax.rem(z + nz - 1, nz) * 2 + c
    mate = z * 2 + (1 - c)
    side = (right, left)

    def at_z(offset):
        return lax.rem(z + nz + offset, nz)

    barrier = pltpu.get_barrier_semaphore()
    for peer in (mate, right, left):
        pl.semaphore_signal(barrier, inc=1, device_id={'sp': peer}, device_id_type=pl.DeviceIdType.MESH)

    def load_x(u):
        return pltpu.make_async_copy(x_hbm.at[u], x_v.at[u], x_sem.at[u])

    first = pl.multiple_of(me * seq, seq)
    loads = [
        pltpu.make_async_copy(wt1_hbm.at[pl.ds(first, seq), :], wt1_v, w_sem.at[0]),
        pltpu.make_async_copy(wt2_hbm.at[:, pl.ds(first, seq)], wt2_v, w_sem.at[1]),
        pltpu.make_async_copy(w1_hbm, w1, w_sem.at[2]),
        pltpu.make_async_copy(w2_hbm, w2, w_sem.at[3]),
    ]
    loads[0].start()
    for u in range(units):
        load_x(u).start()
    for load in loads[1:]:
        load.start()

    def remote(src, dst, slot, u, recv, peer):
        return pltpu.make_async_remote_copy(
            src_ref=src, dst_ref=dst, send_sem=send_sem.at[slot, lax.rem(u, 2)], recv_sem=recv,
            device_id={'sp': peer}, device_id_type=pl.DeviceIdType.MESH)

    def pair_copy(u):
        rows = pl.ds(pl.multiple_of((1 - c) * half_rows, half_rows), half_rows)
        return remote(h_v.at[u, rows, :], d2d_v.at[u], 0, u, dr_sem.at[u], mate)

    def piece_rows(home, lo, n):
        return pl.ds(pl.multiple_of(c * half_rows + home * piece + lo, 8), n)

    def sum_part(way, k):
        if k > 1:
            return 0, piece
        return (0 if way == 0 else piece // 2), piece // 2

    def sum_home(way, k):
        return at_z(hop + 1 - k) if way == 0 else at_z(-(hop + 1 - k))

    def sum_copy(u, way, k):
        lo, n = sum_part(way, k)
        return remote(h_v.at[u, piece_rows(sum_home(way, k), lo, n), :], rs_v.at[u, way, k - 1, pl.ds(lo, n), :],
                      1 + way * hop + k - 1, u, rr_sem.at[u, way, k - 1], side[way])

    def gather_cols(way, k):
        if k < hop:
            return pl.ds(0, ch)
        return pl.ds(0 if way == 0 else ch // 2, ch // 2)

    def gather_copy(u, way, k, shift):
        d = k - 1 + shift
        home = at_z(-d) if way == 0 else at_z(d)
        rows = pl.ds(pl.multiple_of(c * half_rows + home * piece, piece), piece)
        ref = g_v.at[u, rows, gather_cols(way, k)]
        return remote(ref, ref, 1 + 2 * hop + way * hop + k - 1, u, ar_sem.at[u, way, k - 1], side[way])

    def share_copy(u, core):
        rows = pl.ds(pl.multiple_of(core * half_rows, half_rows), half_rows)
        ref = g_v.at[u, rows, :]
        return remote(ref, ref, 1 + 4 * hop, u, gr_sem.at[u], mate)

    def launch(u, copy):
        @pl.when(u >= 2)
        def _():
            copy.wait_send()
        copy.start()

    def project(u):
        load_x(u).wait()
        norm_and_project(x_v.at[u], ln1s, ln1b, wt1t, u_s, h_v.at[u])

    def own_rows():
        return pl.ds(pl.multiple_of(c * half_rows, half_rows), half_rows)

    def add_stage(u, s):
        if s == 1:
            pair_copy(u).wait_recv()
            h_v[u, own_rows(), :] = h_v[u, own_rows(), :] + d2d_v[u]
        elif s <= hop:
            for way in range(2):
                k = s - 1
                sum_copy(u, way, k).wait_recv()
                lo, n = sum_part(way, k)
                rows = piece_rows(sum_home(way, s), lo, n)
                h_v[u, rows, :] = h_v[u, rows, :] + rs_v[u, way, k - 1, lo:lo + n, :]
        elif s == hop + 1:
            for way in range(2):
                sum_copy(u, way, hop).wait_recv()
            rows = piece_rows(z, 0, piece)
            total = h_v[u, rows, :] + rs_v[u, 0, hop - 1] + rs_v[u, 1, hop - 1] + lanes(bcol1[rows, :], ch)
            g_v[u, pl.ds(pl.multiple_of(c * half_rows + z * piece, piece), piece), :] = gelu_of_half(0.5 * total).astype(BF16)
        else:
            for way in range(2):
                gather_copy(u, way, s - hop - 1, 1).wait_recv()

    def send_stage(u, s):
        if s <= hop:
            for way in range(2):
                launch(u, sum_copy(u, way, s))
        elif s <= 2 * hop:
            for way in range(2):
                launch(u, gather_copy(u, way, s - hop, 0))
        else:
            launch(u, share_copy(u, c))

    last_stage = 2 * hop + 2

    def store_out(u):
        return pltpu.make_async_copy(o_v.at[lax.rem(u, 2)], out_hbm.at[u], o_sem.at[lax.rem(u, 2)])

    def mix(u):
        share_copy(u, 1 - c).wait_recv()

        @pl.when(u >= 2)
        def _():
            store_out(u).wait()
        token_out_and_channel_mix(x_v.at[u], g_v.at[u], wt2t, bcol2, ln2s, ln2b, w1, b1h, w2, b2,
                                  x1_s, v_s, q_s, o_v.at[lax.rem(u, 2)])
        store_out(u).start()

    bcol1[...] = column(bt1[...])
    bcol2[...] = column(bt2[:, pl.ds(first, seq)])
    b1h[...] = 0.5 * b1[...]
    loads[0].wait()
    wt1t[...] = wt1_v[...].astype(F32).T.astype(BF16)
    project(0)
    pl.semaphore_wait(barrier, 3)
    pair_copy(0).start()
    project(1)
    pair_copy(1).start()
    loads[1].wait()
    wt2t[...] = wt2_v[...].astype(F32).T.astype(BF16)
    loads[2].wait()
    for r in range(0, ch, 128):
        w1[r:r + 128, :] = (w1[r:r + 128, :].astype(F32) * 0.5).astype(BF16)
    loads[3].wait()

    def tick(t, carry):
        for s in range(1, last_stage):
            u = t - s

            @pl.when(jnp.logical_and(u >= 0, u < units))
            def _(u=u, s=s):
                add_stage(u, s)
        for s in range(1, last_stage):
            u = t - s

            @pl.when(jnp.logical_and(u >= 0, u < units))
            def _(u=u, s=s):
                send_stage(u, s)

        @pl.when(2 * t < units)
        def _():
            for i in range(2):
                u = 2 * t + i
                project(u)
                launch(u, pair_copy(u))

        @pl.when(t >= last_stage)
        def _():
            mix(t - last_stage)
        return carry

    lax.fori_loop(1, units + last_stage, tick, 0)

    for u in (units - 2, units - 1):
        store_out(u).wait()
        pair_copy(u).wait_send()
        share_copy(u, c).wait_send()
        for way in range(2):
            for k in range(1, hop + 1):
                sum_copy(u, way, k).wait_send()
                gather_copy(u, way, k, 0).wait_send()


def fused_layer(nz, patches, ln1_scale, ln1_bias, w_tok1, b_tok1, w_tok2, b_tok2, ln2_scale, ln2_bias, w_ch1, b_ch1, w_ch2, b_ch2):
    units, seq, ch = patches.shape
    tok_hid = w_tok1.shape[1]
    hid = w_ch1.shape[1]
    hop = nz // 2
    piece = tok_hid // 2 // nz
    hbm = pl.BlockSpec(memory_space=pltpu.HBM)
    vmem = pl.BlockSpec(memory_space=pltpu.VMEM)
    row = lambda a: a.reshape(1, -1)
    return pl.pallas_call(
        functools.partial(fused_kernel, nz),
        out_shape=jax.ShapeDtypeStruct(patches.shape, BF16),
        in_specs=[hbm, vmem, vmem, hbm, vmem, hbm, vmem, vmem, vmem, hbm, vmem, hbm, vmem],
        out_specs=hbm,
        scratch_shapes=[
            pltpu.VMEM((units, seq, ch), BF16),
            pltpu.VMEM((units, tok_hid, ch), F32),
            pltpu.VMEM((units, tok_hid // 2, ch), F32),
            pltpu.VMEM((units, 2, hop, piece, ch), F32),
            pltpu.VMEM((units, tok_hid, ch), BF16),
            pltpu.VMEM((seq, tok_hid), BF16),
            pltpu.VMEM((tok_hid, seq), BF16),
            pltpu.VMEM((tok_hid, seq), BF16),
            pltpu.VMEM((seq, tok_hid), BF16),
            pltpu.VMEM((tok_hid, 128), F32),
            pltpu.VMEM((seq, 128), F32),
            pltpu.VMEM((ch, hid), BF16),
            pltpu.VMEM((hid, ch), BF16),
            pltpu.VMEM((1, hid), F32),
            pltpu.VMEM((seq, ch), BF16),
            pltpu.VMEM((seq, ch), BF16),
            pltpu.VMEM((seq, ch), BF16),
            pltpu.VMEM((seq, hid), BF16),
            pltpu.VMEM((2, seq, ch), BF16),
            pltpu.SemaphoreType.DMA((units,)),
            pltpu.SemaphoreType.DMA((4,)),
            pltpu.SemaphoreType.DMA((2,)),
            pltpu.SemaphoreType.DMA((2 + 4 * hop, 2)),
            pltpu.SemaphoreType.DMA((units,)),
            pltpu.SemaphoreType.DMA((units, 2, hop)),
            pltpu.SemaphoreType.DMA((units, 2, hop)),
            pltpu.SemaphoreType.DMA((units,)),
        ],
        compiler_params=pltpu.CompilerParams(collective_id=0, has_side_effects=True, vmem_limit_bytes=VMEM_LIMIT),
    )(patches, row(ln1_scale), row(ln1_bias), w_tok1, row(b_tok1), w_tok2, row(b_tok2),
      row(ln2_scale), row(ln2_bias), w_ch1, row(b_ch1), w_ch2, row(b_ch2))


def solution(mesh):
    row_spec = P('dp', 'sp', None)
    full_spec = P()
    nz = mesh.shape['sp'] // 2
    return jax.shard_map(functools.partial(fused_layer, nz), mesh=mesh, in_specs=(row_spec,) + (full_spec,) * 12,
                         out_specs=row_spec, check_vma=False)
```

```python
import functools

import jax
import jax.numpy as jnp
from jax import lax
from jax.experimental import pallas as pl
from jax.experimental.pallas import tpu as pltpu
from jax.sharding import PartitionSpec as P

LN_EPS = 1e-6
GELU_K = 0.7978845608028654
F32 = jnp.float32
BF16 = jnp.bfloat16
VMEM_LIMIT = 67043328
PAIR_SLOTS = 2
HOP_SLOTS = 3


def layer_norm(wide, scale, offset):
    mean = jnp.mean(wide, axis=-1, keepdims=True)
    centered = wide - mean
    var = jnp.mean(centered * centered, axis=-1, keepdims=True)
    return (centered * lax.rsqrt(var + LN_EPS) * scale + offset).astype(BF16)


def gelu_of_half(half):
    inner = half * (half * half * (8.0 * 0.044715 * GELU_K) + 2.0 * GELU_K)
    return half + half * jnp.tanh(inner)


def lanes(col, width):
    return jnp.concatenate([col] * (width // 128), axis=1)


def column(row):
    return jnp.broadcast_to(row, (128, row.shape[1])).T


def norm_and_project(x_img, ln1s, ln1b, wt1t, u_s, h_img):
    seq, ch = u_s.shape
    step = 128
    for r in range(0, seq, step):
        u_s[r:r + step, :] = layer_norm(x_img[r:r + step, :].astype(F32), ln1s[...], ln1b[...])
    h_img[...] = jnp.dot(wt1t[...], u_s[...], preferred_element_type=F32)


def token_out_and_channel_mix(x_img, g_img, wt2t, bcol2, ln2s, ln2b, w1, b1h, w2, b2, x1_s, v_s, q_s, o_img, first=0, count=None, rows=256, wide=512):
    seq, ch = v_s.shape
    hid = w1.shape[1]
    for r in range(first, first + (count or seq), rows):
        rs = slice(r, r + rows)
        mixed = jnp.dot(wt2t[rs, :], g_img[...], preferred_element_type=F32)
        mixed = (mixed + lanes(bcol2[rs, :], ch)).astype(BF16)
        x1 = (x_img[rs, :].astype(F32) + mixed.astype(F32)).astype(BF16)
        x1_s[rs, :] = x1
        v_s[rs, :] = layer_norm(x1.astype(F32), ln2s[...], ln2b[...])
        for e in range(0, hid, wide):
            es = slice(e, e + wide)
            half = jnp.dot(v_s[rs, :], w1[:, es], preferred_element_type=F32) + b1h[:, es]
            q_s[rs, es] = gelu_of_half(half).astype(BF16)
        y = jnp.dot(q_s[rs, :], w2[...], preferred_element_type=F32) + b2[...]
        o_img[rs, :] = (x1_s[rs, :].astype(F32) + y).astype(BF16)


def fused_kernel(nz, x_hbm, ln1s, ln1b, wt1_hbm, bt1, wt2_hbm, bt2, ln2s, ln2b, w1_hbm, b1, w2_hbm, b2, out_hbm,
                 x_v, h_v, d2d_v, rs_v, g_v, wt1_v, wt1t, wt2_v, wt2t, bcol1, bcol2, w1, w2, b1h, u_s, x1_s, v_s, q_s, o_v,
                 x_sem, w_sem, o_sem, send_sem, dr_sem, rr_sem, ar_sem, gr_sem):
    units, seq, ch = x_v.shape
    tok_hid = h_v.shape[1]
    hid = w1.shape[1]
    half_rows = tok_hid // 2
    piece = half_rows // nz
    hop = nz // 2
    me = lax.axis_index('sp')
    z = lax.div(me, 2)
    c = lax.rem(me, 2)
    right = lax.rem(z + 1, nz) * 2 + c
    left = lax.rem(z + nz - 1, nz) * 2 + c
    mate = z * 2 + (1 - c)
    side = (right, left)

    half_base = pl.multiple_of(c * half_rows, half_rows)
    other_base = pl.multiple_of((1 - c) * half_rows, half_rows)
    piece_base = [pl.multiple_of(c * half_rows + lax.rem(z + i, nz) * piece, piece) for i in range(nz)]

    def base_at(distance):
        return piece_base[distance % nz]

    barrier = pltpu.get_barrier_semaphore()
    for peer in (mate, right, left):
        pl.semaphore_signal(barrier, inc=1, device_id={'sp': peer}, device_id_type=pl.DeviceIdType.MESH)

    def load_x(u):
        return pltpu.make_async_copy(x_hbm.at[u], x_v.at[u], x_sem.at[u])

    first = pl.multiple_of(me * seq, seq)
    loads = [
        pltpu.make_async_copy(wt1_hbm.at[pl.ds(first, seq), :], wt1_v, w_sem.at[0]),
        pltpu.make_async_copy(wt2_hbm.at[:, pl.ds(first, seq)], wt2_v, w_sem.at[1]),
        pltpu.make_async_copy(w1_hbm, w1, w_sem.at[2]),
        pltpu.make_async_copy(w2_hbm, w2, w_sem.at[3]),
    ]
    loads[0].start()
    for u in range(units):
        load_x(u).start()
    for load in loads[1:]:
        load.start()

    def remote(src, dst, slot, recv, peer):
        return pltpu.make_async_remote_copy(
            src_ref=src, dst_ref=dst, send_sem=send_sem.at[slot], recv_sem=recv,
            device_id={'sp': peer}, device_id_type=pl.DeviceIdType.MESH)

    def pair_copy(u):
        return remote(h_v.at[u, pl.ds(other_base, half_rows), :], d2d_v.at[u], 0, dr_sem.at[u], mate)

    def sum_part(way, k):
        if k > 1:
            return 0, piece
        return (0 if way == 0 else piece // 2), piece // 2

    def sum_rows(way, k, lo, n):
        base = base_at(hop + 1 - k if way == 0 else k - hop - 1)
        return pl.ds(base if lo == 0 else pl.multiple_of(base + lo, 8), n)

    def sum_copy(u, way, k):
        lo, n = sum_part(way, k)
        return remote(h_v.at[u, sum_rows(way, k, lo, n), :], rs_v.at[u, way, k - 1, pl.ds(lo, n), :],
                      1 + way * hop + k - 1, rr_sem.at[u, way, k - 1], side[way])

    def gather_cols(way, k):
        if k < hop:
            return pl.ds(0, ch)
        return pl.ds(0 if way == 0 else ch // 2, ch // 2)

    def gather_copy(u, way, k, shift):
        d = k - 1 + shift
        ref = g_v.at[u, pl.ds(base_at(-d if way == 0 else d), piece), gather_cols(way, k)]
        return remote(ref, ref, 1 + 2 * hop + way * hop + k - 1, ar_sem.at[u, way, k - 1], side[way])

    def share_copy(u, base):
        ref = g_v.at[u, pl.ds(base, half_rows), :]
        return remote(ref, ref, 1 + 4 * hop, gr_sem.at[u], mate)

    def all_sent():
        def sent(ref, slot):
            remote(ref, ref, slot, dr_sem.at[0], mate).wait_send()
        sent(d2d_v, 0)
        sent(g_v.at[:, pl.ds(0, half_rows), :], 1 + 4 * hop)
        for way in range(2):
            for k in range(1, hop + 1):
                lo, n = sum_part(way, k)
                sent(rs_v.at[:, way, k - 1, pl.ds(lo, n), :], 1 + way * hop + k - 1)
                sent(g_v.at[:, pl.ds(0, piece), gather_cols(way, k)], 1 + 2 * hop + way * hop + k - 1)

    def project(u):
        load_x(u).wait()
        norm_and_project(x_v.at[u], ln1s, ln1b, wt1t, u_s, h_v.at[u])

    def serve_stage(u, s):
        if s == 1:
            pair_copy(u).wait_recv()
            rows = pl.ds(half_base, half_rows)
            h_v[u, rows, :] = h_v[u, rows, :] + d2d_v[u]
        elif s <= hop:
            for way in range(2):
                sum_copy(u, way, s - 1).wait_recv()
            for way in range(2):
                lo, n = sum_part(way, s - 1)
                rows = sum_rows(way, s, lo, n)
                h_v[u, rows, :] = h_v[u, rows, :] + rs_v[u, way, s - 2, lo:lo + n, :]
        elif s == hop + 1:
            for way in range(2):
                sum_copy(u, way, hop).wait_recv()
            rows = pl.ds(base_at(0), piece)
            total = h_v[u, rows, :] + rs_v[u, 0, hop - 1] + rs_v[u, 1, hop - 1] + lanes(bcol1[rows, :], ch)
            g_v[u, rows, :] = gelu_of_half(0.5 * total).astype(BF16)
        else:
            for way in range(2):
                gather_copy(u, way, s - hop - 1, 1).wait_recv()
        if s <= hop:
            for way in range(2):
                sum_copy(u, way, s).start()
        elif s <= 2 * hop:
            for way in range(2):
                gather_copy(u, way, s - hop, 0).start()
        else:
            share_copy(u, half_base).start()

    last_stage = 2 * hop + 2
    delay = [0, PAIR_SLOTS]
    for s in range(2, last_stage):
        delay.append(delay[-1] + HOP_SLOTS)
    fill = (delay[-1] + PAIR_SLOTS + 1) // 2

    def store_out(u):
        return pltpu.make_async_copy(o_v.at[lax.rem(u, 2)], out_hbm.at[u], o_sem.at[lax.rem(u, 2)])

    def serve(t, p):
        due = [(s, t - delay[s] // 2) for s in range(last_stage - 1, 0, -1) if delay[s] % 2 == p]
        for s, u in due:
            @pl.when(jnp.logical_and(u >= 0, u < units))
            def _(u=u, s=s):
                serve_stage(u, s)

    def mix_half(u, p):
        if p == 0:
            share_copy(u, other_base).wait_recv()

            @pl.when(u >= 2)
            def _():
                store_out(u).wait()
        token_out_and_channel_mix(x_v.at[u], g_v.at[u], wt2t, bcol2, ln2s, ln2b, w1, b1h, w2, b2,
                                  x1_s, v_s, q_s, o_v.at[lax.rem(u, 2)], first=p * (seq // 2), count=seq // 2)
        if p == 1:
            store_out(u).start()

    loads[0].wait()
    wt1t[...] = wt1_v[...].astype(F32).T.astype(BF16)
    project(0)
    pl.semaphore_wait(barrier, 3)
    pair_copy(0).start()
    bcol1[...] = column(bt1[...])

    def prepare_weights():
        bcol2[...] = column(bt2[:, pl.ds(first, seq)])
        b1h[...] = 0.5 * b1[...]
        loads[1].wait()
        wt2t[...] = wt2_v[...].astype(F32).T.astype(BF16)
        loads[2].wait()
        for r in range(0, ch, 128):
            w1[r:r + 128, :] = (w1[r:r + 128, :].astype(F32) * 0.5).astype(BF16)
        loads[3].wait()

    def fill_tick(t, carry):
        for p in range(2):
            serve(t, p)
            u = 2 * t + p

            @pl.when(jnp.logical_and(u >= 1, u < units))
            def _(u=u):
                project(u)
                pair_copy(u).start()
        pl.when(t == units // 2)(prepare_weights)
        return carry

    def main_tick(t, carry):
        for p in range(2):
            serve(t, p)
            mix_half(t - fill, p)
        return carry

    lax.fori_loop(0, fill, fill_tick, 0)
    lax.fori_loop(fill, fill + units, main_tick, 0)

    for u in (units - 2, units - 1):
        store_out(u).wait()
    all_sent()


def fused_layer(nz, patches, ln1_scale, ln1_bias, w_tok1, b_tok1, w_tok2, b_tok2, ln2_scale, ln2_bias, w_ch1, b_ch1, w_ch2, b_ch2):
    units, seq, ch = patches.shape
    tok_hid = w_tok1.shape[1]
    hid = w_ch1.shape[1]
    hop = nz // 2
    piece = tok_hid // 2 // nz
    hbm = pl.BlockSpec(memory_space=pltpu.HBM)
    vmem = pl.BlockSpec(memory_space=pltpu.VMEM)
    row = lambda a: a.reshape(1, -1)
    return pl.pallas_call(
        functools.partial(fused_kernel, nz),
        out_shape=jax.ShapeDtypeStruct(patches.shape, BF16),
        in_specs=[hbm, vmem, vmem, hbm, vmem, hbm, vmem, vmem, vmem, hbm, vmem, hbm, vmem],
        out_specs=hbm,
        scratch_shapes=[
            pltpu.VMEM((units, seq, ch), BF16),
            pltpu.VMEM((units, tok_hid, ch), F32),
            pltpu.VMEM((units, tok_hid // 2, ch), F32),
            pltpu.VMEM((units, 2, hop, piece, ch), F32),
            pltpu.VMEM((units, tok_hid, ch), BF16),
            pltpu.VMEM((seq, tok_hid), BF16),
            pltpu.VMEM((tok_hid, seq), BF16),
            pltpu.VMEM((tok_hid, seq), BF16),
            pltpu.VMEM((seq, tok_hid), BF16),
            pltpu.VMEM((tok_hid, 128), F32),
            pltpu.VMEM((seq, 128), F32),
            pltpu.VMEM((ch, hid), BF16),
            pltpu.VMEM((hid, ch), BF16),
            pltpu.VMEM((1, hid), F32),
            pltpu.VMEM((seq, ch), BF16),
            pltpu.VMEM((seq, ch), BF16),
            pltpu.VMEM((seq, ch), BF16),
            pltpu.VMEM((seq, hid), BF16),
            pltpu.VMEM((2, seq, ch), BF16),
            pltpu.SemaphoreType.DMA((units,)),
            pltpu.SemaphoreType.DMA((4,)),
            pltpu.SemaphoreType.DMA((2,)),
            pltpu.SemaphoreType.DMA((2 + 4 * hop,)),
            pltpu.SemaphoreType.DMA((units,)),
            pltpu.SemaphoreType.DMA((units, 2, hop)),
            pltpu.SemaphoreType.DMA((units, 2, hop)),
            pltpu.SemaphoreType.DMA((units,)),
        ],
        compiler_params=pltpu.CompilerParams(collective_id=0, has_side_effects=True, vmem_limit_bytes=VMEM_LIMIT),
    )(patches, row(ln1_scale), row(ln1_bias), w_tok1, row(b_tok1), w_tok2, row(b_tok2),
      row(ln2_scale), row(ln2_bias), w_ch1, row(b_ch1), w_ch2, row(b_ch2))


def solution(mesh):
    row_spec = P('dp', 'sp', None)
    full_spec = P()
    nz = mesh.shape['sp'] // 2
    return jax.shard_map(functools.partial(fused_layer, nz), mesh=mesh, in_specs=(row_spec,) + (full_spec,) * 12,
                         out_specs=row_spec, check_vma=False)
```
